32 devices in a mesh: seq: 8 (over z, x), head: 4 (over y, core).
Axes of the slice: x: 2, y: 2, z: 4, core: 2. Of those that a mesh axis runs over, the one named last changes fastest.
Arguments:
- queries: bfloat16 [4096, 6144], P('seq', 'head'), may hold values from -10 to 10
- keys: bfloat16 [4096, 6144], P('seq', 'head'), may hold values from -10 to 10
- values: bfloat16 [4096, 6144], P('seq', 'head'), may hold values from -6 to 6
- frame_of_block: int32 [16], P('seq'), may hold values from 0 to 7, never falling along the last dimension, each value on 1 to 4 neighbouring positions
- pair_mask: int32 [16, 16], P('seq'), may hold values 0 or 1
- w_out: bfloat16 [6144, 6144], P('head', 'seq'), may hold values from -0.4375 to 0.4375
Outputs:
- projected: bfloat16 [4096, 6144], P('seq', 'head')
The draws below stay inside these ranges and needn't reach their ends.
Inputs may be any that keep to these rules, and one draw needn't show every extreme that they name: `frame_of_block`: frame ids never fall along the blocks, every frame spans 1 to 4 consecutive blocks.
All inputs are finite; a program needn't handle non-finite values. No bound on the sum of `pair_mask` on one device may be relied on, other than what follows from the above.
Results may differ from the reference program's by a relative error of at most 0.015.
Values may be sent and summed in bfloat16 or wider, within the bound.
A program may use at most 192 MiB of HBM per device.

```python
import math
import jax
import jax.numpy as jnp
import numpy as np
from jax import lax

D = 6144
H = 48
HD = 128
BLK = 256
TOK_DEV = 512
TOKENS = 4096
NBLK = 16
FRAMES = 8


def joint_draw(key):
    width = H * HD
    q_draw = jnp.clip(1.5 * jax.random.normal(jax.random.fold_in(key, 101), (TOKENS, width), jnp.float32), -6.0, 6.0)
    k_draw = jnp.clip(1.5 * jax.random.normal(jax.random.fold_in(key, 202), (TOKENS, width), jnp.float32), -6.0, 6.0)
    return (q_draw, k_draw)


def draw_queries(key, part):
    return joint_draw(key)[0].astype(jnp.bfloat16)


def draw_keys(key, part):
    return joint_draw(key)[1].astype(jnp.bfloat16)


def touch_ends(result, stream_key, least, largest):
    spot = [jax.random.randint(jax.random.fold_in(stream_key, axis), (), 0, length) for axis, length in enumerate(result.shape)]
    main_axis = result.shape.index(max(result.shape))
    beside = spot[:main_axis] + [(spot[main_axis] + 1) % result.shape[main_axis]] + spot[main_axis + 1:]
    return result.at[tuple(spot)].set(least).at[tuple(beside)].set(largest)


def shard_levels(own_key, extent, shards, low, largest):
    factor_of, own = 1.0, jax.random.fold_in(own_key, 6)
    for dim, parts in shards:
        steps = jnp.exp(jax.random.uniform(jax.random.fold_in(own, dim), (parts,), jnp.float32, low / len(shards), largest / len(shards)))
        factor_of = factor_of * jnp.repeat(steps, extent[dim] // parts).reshape([-1 if axis == dim else 1 for axis in range(len(extent))])
    return factor_of


def length_profile(count, total, most, slope):
    weights = [(1 << 20) // math.isqrt(standing ** slope) + 1 for standing in range(2, count + 1)]
    spare, given = total - most - (count - 1), [1] * (count - 1)
    while spare > 0:
        movable = [i for i in range(count - 1) if given[i] < most]
        mass, left = sum([weights[i] for i in movable]), spare
        for i in movable:
            more = min(most - given[i], max(1, left * weights[i] // mass), spare)
            given[i] = given[i] + more
            spare = spare - more
    return np.array([most] + given)


def uneven_parts(key, amount, total, reach, skew):
    if amount == 2:
        one = jax.random.randint(key, (), max(1, total - reach), min(reach, total - 1) + 1)
        return jnp.stack([one, total - one])
    tallies = jnp.asarray(length_profile(amount, total, reach, skew), jnp.int32)
    twos = (amount - 1) // 2
    giver, sink = tallies[1:1 + 2 * twos:2], tallies[2:2 + 2 * twos:2]
    slack = jnp.minimum(giver - 1, reach - sink)
    shifted = jax.random.randint(jax.random.fold_in(key, 1), (twos,), 0, 1 << 20) % (slack + 1)
    tallies = tallies.at[1:1 + 2 * twos:2].set(giver - shifted).at[2:2 + 2 * twos:2].set(sink + shifted)
    return tallies[jax.random.permutation(jax.random.fold_in(key, 2), amount)]


def noise(stream_key, dims, scale, most, pieces=(), kind=jnp.bfloat16):
    values = scale * jax.random.normal(stream_key, dims, jnp.float32)
    if pieces:
        values = values * shard_levels(stream_key, dims, pieces, -0.22, 0.18)
    return jnp.clip(values, -most, most).astype(kind)


def setup_inputs(seed: int = 0) -> dict:
    key_of = jax.random.split(jax.random.key(seed), 7)
    return {
        "queries": draw_queries(jax.random.fold_in(key_of[6], 71), 0),
        "keys": draw_keys(jax.random.fold_in(key_of[6], 71), 0),
        "values": noise(key_of[2], (TOKENS, D), 1.0, 6.0, ((0, 8), (1, 4))),
        "frame_of_block": jnp.searchsorted(jnp.cumsum(uneven_parts(key_of[3], FRAMES, NBLK, 4, 1)), jnp.arange(NBLK), side="right").astype(jnp.int32),
        "pair_mask": touch_ends((jax.random.randint(key_of[4], (NBLK, NBLK), 0, 4) < 3).astype(jnp.int32), jax.random.fold_in(key_of[4], 1), 0, 1),
        "w_out": noise(key_of[5], (D, D), (D // 32) ** -0.5, 0.4375, ((0, 4), (1, 8))),
    }


def reference(queries, keys, values, frame_of_block, pair_mask, w_out):
    width = H * HD
    scale = 1.0 / math.sqrt(HD)
    tok_frame = jnp.repeat(frame_of_block, BLK)
    key_block = (jnp.arange(TOKENS, dtype=jnp.int32) // BLK).astype(jnp.int32)
    count_blocks = TOKENS // TOK_DEV

    def one_block(index):
        first = (index * TOK_DEV).astype(jnp.int32)
        rows = lax.dynamic_slice_in_dim(queries, first, TOK_DEV, 0)
        q_frame = lax.dynamic_slice_in_dim(tok_frame, first, TOK_DEV, 0)
        q_block = ((first + jnp.arange(TOK_DEV, dtype=jnp.int32)) // BLK).astype(jnp.int32)
        link = pair_mask[q_block][:, key_block]
        allowed = (tok_frame[None, :] <= q_frame[:, None]) & ((link == 1) | (tok_frame[None, :] == q_frame[:, None]))

        def one_head(head_index):
            col = (head_index * HD).astype(jnp.int32)
            q_head = lax.dynamic_slice_in_dim(rows, col, HD, 1)
            k_head = lax.dynamic_slice_in_dim(keys, col, HD, 1)
            v_head = lax.dynamic_slice_in_dim(values, col, HD, 1)
            score = jnp.dot(q_head, k_head.T, preferred_element_type=jnp.float32) * scale
            score = jnp.where(allowed, score, -1e+30)
            peak = lax.optimization_barrier(jnp.max(score, axis=1))
            weight = jnp.where(allowed, jnp.exp(score - peak[:, None]), 0.0)
            total = lax.optimization_barrier(jnp.sum(weight, axis=1))
            mixed = jnp.dot(weight.astype(jnp.bfloat16), v_head, preferred_element_type=jnp.float32)
            return mixed / total[:, None]
        heads = lax.map(one_head, jnp.arange(H, dtype=jnp.int32))
        return jnp.transpose(heads, (1, 0, 2)).reshape(TOK_DEV, width).astype(jnp.bfloat16)
    attn = lax.map(one_block, jnp.arange(count_blocks, dtype=jnp.int32)).reshape(TOKENS, width)
    return jnp.dot(attn, w_out, preferred_element_type=jnp.float32).astype(jnp.bfloat16)
```

```python
import functools
import math

import jax
import jax.numpy as jnp
from jax import lax
from jax.experimental import pallas as pl
from jax.experimental.pallas import tpu as pltpu
from jax.sharding import PartitionSpec as P

HD = 128
BLK = 256
NEG = -1e30


def body_gather(queries, keys, values, frame_of_block, pair_mask, w_out):
    tok = queries.shape[0]
    heads_here = queries.shape[1] // HD
    count_blocks = pair_mask.shape[1]
    scale = 1.0 / math.sqrt(HD)
    key_span = 512
    q_heads = queries.reshape(tok, heads_here, HD)
    q_frame = jnp.repeat(frame_of_block, BLK)
    mask_rows = jnp.repeat(pair_mask.astype(jnp.float32), BLK, axis=0)
    block_ids = jnp.arange(count_blocks, dtype=jnp.int32)

    def update(state, k_rows, v_rows, allowed):
        peak, total, accum = state
        k_heads = k_rows.reshape(k_rows.shape[0], heads_here, HD)
        v_heads = v_rows.reshape(v_rows.shape[0], heads_here, HD)
        score = (
            jnp.einsum("qhd,khd->hqk", q_heads, k_heads, preferred_element_type=jnp.float32) * scale
        )
        score = jnp.where(allowed[None], score, -1e30)
        new_peak = jnp.maximum(peak, jnp.max(score, axis=2))
        weight = jnp.where(allowed[None], jnp.exp(score - new_peak[:, :, None]), 0.0)
        factor = jnp.exp(peak - new_peak)
        new_total = total * factor + jnp.sum(weight, axis=2)
        added = jnp.einsum(
            "hqk,khd->qhd", weight.astype(jnp.bfloat16), v_heads, preferred_element_type=jnp.float32
        )
        new_accum = accum * factor.T[:, :, None] + added
        return (new_peak, new_total, new_accum)

    def attend_block(state, k_rows, v_rows, k_frame, start):
        count = k_rows.shape[0]
        k_block = (start + jnp.arange(count, dtype=jnp.int32)) // BLK
        one_hot = (block_ids[:, None] == k_block[None, :]).astype(jnp.float32)
        link = jnp.dot(mask_rows, one_hot, preferred_element_type=jnp.float32)
        same = k_frame[None, :] == q_frame[:, None]
        allowed = (k_frame[None, :] <= q_frame[:, None]) & ((link > 0.5) | same)
        return update(state, k_rows, v_rows, allowed)

    initial = (
        jnp.full((heads_here, tok), -1e30, jnp.float32),
        jnp.zeros((heads_here, tok), jnp.float32),
        jnp.zeros((tok, heads_here, HD), jnp.float32),
    )
    k_frame_local = jnp.repeat(frame_of_block, BLK)
    k_rows = lax.all_gather(keys, "seq", axis=0, tiled=True)
    v_rows = lax.all_gather(values, "seq", axis=0, tiled=True)
    k_frame = lax.all_gather(k_frame_local, "seq", axis=0, tiled=True)
    count = k_rows.shape[0]

    def step(index, inner):
        offset = (index * key_span).astype(jnp.int32)
        return attend_block(
            inner,
            lax.dynamic_slice_in_dim(k_rows, offset, key_span, 0),
            lax.dynamic_slice_in_dim(v_rows, offset, key_span, 0),
            lax.dynamic_slice_in_dim(k_frame, offset, key_span, 0),
            offset,
        )

    state = lax.fori_loop(0, count // key_span, step, initial)
    peak, total, accum = state
    attn = (accum / total.T[:, :, None]).reshape(tok, heads_here * HD).astype(jnp.bfloat16)
    terms = jnp.dot(
        attn, lax.all_gather(w_out, "seq", axis=1, tiled=True), preferred_element_type=jnp.float32
    )
    return lax.psum_scatter(terms.astype(jnp.bfloat16), "head", scatter_dimension=1, tiled=True)


def greet(n, me):
    barrier = pltpu.get_barrier_semaphore()
    for k in range(1, n):
        pl.semaphore_signal(barrier, inc=1, device_id={"seq": lax.rem(me + k, n)}, device_id_type=pl.DeviceIdType.MESH)
    pl.semaphore_wait(barrier, n - 1)


def cols(head):
    return pl.ds(pl.multiple_of(head * HD, HD), HD)


def rows(start, size):
    return pl.ds(pl.multiple_of(start, size), size)


def spread_kernel(n, tok, q, k, v, meta, qf, qs, kf, ks, vf, vs, metas, hold, hold_half, hold_meta, send, recv, here):
    me = lax.axis_index("seq")
    half = tok // 2

    def pieces(to):
        pair, odd = to // 2, lax.rem(to, 2)
        own, shared = cols(3 * pair + 2 * odd), cols(3 * pair + 1)
        full = rows(me * tok, tok)
        return [
            (meta, metas.at[rows(me * 8, 8)]),
            (q.at[:, own], qf.at[full]),
            (k.at[:, own], kf.at[full]),
            (v.at[:, own], vf.at[full]),
            (q.at[rows(odd * half, half), shared], qs.at[rows(me * half, half)]),
            (k.at[:, shared], ks.at[full]),
            (v.at[:, shared], vs.at[full]),
        ]

    def bounce(index):
        if index == 0:
            return hold_meta
        if index == 4:
            return hold_half
        return hold.at[{1: 0, 2: 1, 3: 2, 5: 3, 6: 4}[index]]

    greet(n, me)
    copies = []
    for step in range(1, n):
        to = lax.rem(me + step, n)
        for i, (src, dst) in enumerate(pieces(to)):
            copy = pltpu.make_async_remote_copy(
                src_ref=src, dst_ref=dst, send_sem=send.at[step - 1, i], recv_sem=recv.at[step - 1, i],
                device_id={"seq": to}, device_id_type=pl.DeviceIdType.MESH,
            )
            copy.start()
            copies.append(copy)
    mine = pieces(me)
    ins = [pltpu.make_async_copy(src, bounce(i), here.at[0, i]) for i, (src, _) in enumerate(mine)]
    outs = [pltpu.make_async_copy(bounce(i), dst, here.at[1, i]) for i, (_, dst) in enumerate(mine)]
    for c in ins:
        c.start()
    for c, d in zip(ins, outs):
        c.wait()
        d.start()
    for d in outs:
        d.wait()
    for c in copies:
        c.wait()


def return_kernel(n, tok, of, os, attn, hold, hold_half, send, recv, here):
    me = lax.axis_index("seq")
    half = tok // 2
    pair, odd = me // 2, lax.rem(me, 2)
    own, shared = cols(3 * pair + 2 * odd), cols(3 * pair + 1)

    def pieces(to):
        return [
            (of.at[rows(to * tok, tok)], attn.at[:, own]),
            (os.at[rows(to * half, half)], attn.at[rows(odd * half, half), shared]),
        ]

    greet(n, me)
    copies = []
    for step in range(1, n):
        to = lax.rem(me + step, n)
        for i, (src, dst) in enumerate(pieces(to)):
            copy = pltpu.make_async_remote_copy(
                src_ref=src, dst_ref=dst, send_sem=send.at[step - 1, i], recv_sem=recv.at[step - 1, i],
                device_id={"seq": to}, device_id_type=pl.DeviceIdType.MESH,
            )
            copy.start()
            copies.append(copy)
    for i, ((src, dst), via) in enumerate(zip(pieces(me), (hold, hold_half))):
        c = pltpu.make_async_copy(src, via, here.at[0, i])
        c.start()
        c.wait()
        d = pltpu.make_async_copy(via, dst, here.at[1, i])
        d.start()
        d.wait()
    for c in copies:
        c.wait()


def attend_kernel(odd_ref, count_ref, list_ref, qf, qs, kf, ks, vf, vs, of, os):
    odd = odd_ref[0]
    j = pl.program_id(0)
    factor = math.log2(math.e) / math.sqrt(HD)

    def scores(q, k):
        return lax.dot_general(q, k, (((1,), (1,)), ((), ())), preferred_element_type=jnp.float32)

    def fold(state, parts, vals):
        peak, total, accum = state
        top = parts[0]
        for s in parts[1:]:
            top = jnp.maximum(top, s)
        new_peak = jnp.maximum(peak, jnp.max(top, axis=1, keepdims=True))
        keep = jnp.exp2((peak - new_peak) * factor)
        total, accum = total * keep, accum * keep
        for s, v in zip(parts, vals):
            p = jnp.exp2((s - new_peak) * factor)
            for c in range(0, BLK, HD):
                total = total + p[:, c:c + HD]
            accum = accum + jnp.dot(p.astype(jnp.bfloat16), v, preferred_element_type=jnp.float32)
        return new_peak, total, accum

    def start():
        return (
            jnp.full((BLK, 1), NEG, jnp.float32),
            jnp.zeros((BLK, HD), jnp.float32),
            jnp.zeros((BLK, HD), jnp.float32),
        )

    def finish(state):
        _, total, accum = state
        return (accum / jnp.sum(total, axis=1, keepdims=True)).astype(jnp.bfloat16)

    def walk(block, streams):
        count = count_ref[block]

        def step(i, states):
            a = rows(list_ref[block, 2 * i] * BLK, BLK)
            b = rows(list_ref[block, 2 * i + 1] * BLK, BLK)
            bias = jnp.where(2 * i + 1 < count, 0.0, NEG).astype(jnp.float32)
            parts = [[scores(q, k[a, :]), scores(q, k[b, :]) + bias] for q, k, _ in streams]
            return tuple(
                fold(state, part, (v[a, :], v[b, :])) for state, part, (_, _, v) in zip(states, parts, streams)
            )

        return lax.fori_loop(0, (count + 1) // 2, step, tuple(start() for _ in streams))

    same, other = rows(odd * BLK, BLK), rows((1 - odd) * BLK, BLK)
    first, second = walk(2 * j + odd, [(qf[same, :], kf, vf), (qs[...], ks, vs)])
    of[same, :] = finish(first)
    os[...] = finish(second)
    (third,) = walk(2 * j + 1 - odd, [(qf[other, :], kf, vf)])
    of[other, :] = finish(third)


def body_spread(n, queries, keys, values, frame_of_block, pair_mask, w_out):
    tok, width = queries.shape
    count_blocks = pair_mask.shape[1]
    tokens = n * tok
    per = tok // BLK
    w_all = lax.all_gather(w_out, "seq", axis=1, tiled=True)
    meta = jnp.concatenate([frame_of_block[:, None], pair_mask], axis=1)
    meta = jnp.pad(meta, ((0, 8 - per), (0, HD - 1 - count_blocks)))
    anyspace = pl.BlockSpec(memory_space=pl.ANY)
    big = jax.ShapeDtypeStruct((tokens, HD), queries.dtype)
    small = jax.ShapeDtypeStruct((tokens // 2, HD), queries.dtype)
    qf, qs, kf, ks, vf, vs, metas = pl.pallas_call(
        functools.partial(spread_kernel, n, tok),
        out_shape=[big, small, big, big, big, big, jax.ShapeDtypeStruct((8 * n, HD), jnp.int32)],
        in_specs=[anyspace] * 4,
        out_specs=[anyspace] * 7,
        scratch_shapes=[
            pltpu.VMEM((5, tok, HD), queries.dtype),
            pltpu.VMEM((tok // 2, HD), queries.dtype),
            pltpu.VMEM((8, HD), jnp.int32),
            pltpu.SemaphoreType.DMA((n - 1, 7)),
            pltpu.SemaphoreType.DMA((n - 1, 7)),
            pltpu.SemaphoreType.DMA((2, 7)),
        ],
        compiler_params=pltpu.CompilerParams(collective_id=0, has_side_effects=True),
        cost_estimate=pl.CostEstimate(flops=0, bytes_accessed=300_000_000, transcendentals=0),
        name="spread",
    )(queries, keys, values, meta)

    metas = metas.reshape(n, 8, HD)[:, :per].reshape(n * per, HD)
    frame, links = metas[:, 0], metas[:, 1:1 + count_blocks]
    allowed = (frame[None, :] <= frame[:, None]) & ((links == 1) | (frame[None, :] == frame[:, None]))
    place = jnp.cumsum(allowed.astype(jnp.int32), axis=1)
    count = place[:, -1]
    ids = jnp.arange(count_blocks, dtype=jnp.int32)
    hit = allowed[:, None, :] & (place[:, None, :] == ids[None, :, None] + 1)
    order = jnp.sum(jnp.where(hit, ids[None, None, :], 0), axis=2)
    odd = lax.rem(lax.axis_index("seq"), 2).reshape(1).astype(jnp.int32)

    smem = pl.BlockSpec(memory_space=pltpu.SMEM)
    whole = pl.BlockSpec((tokens, HD), lambda j: (0, 0))
    two = pl.BlockSpec((2 * BLK, HD), lambda j: (j, 0))
    one = pl.BlockSpec((BLK, HD), lambda j: (j, 0))
    of, os = pl.pallas_call(
        attend_kernel,
        grid=(tokens // (2 * BLK),),
        out_shape=[big, small],
        in_specs=[smem, smem, smem, two, one, whole, whole, whole, whole],
        out_specs=[two, one],
        compiler_params=pltpu.CompilerParams(vmem_limit_bytes=48 * 1024 * 1024),
        cost_estimate=pl.CostEstimate(flops=20_000_000_000, bytes_accessed=8_000_000, transcendentals=20_000_000),
        name="attend",
    )(odd, count, order, qf, qs, kf, ks, vf, vs)

    attn = pl.pallas_call(
        functools.partial(return_kernel, n, tok),
        out_shape=jax.ShapeDtypeStruct((tok, width), queries.dtype),
        in_specs=[anyspace] * 2,
        out_specs=anyspace,
        scratch_shapes=[
            pltpu.VMEM((tok, HD), queries.dtype),
            pltpu.VMEM((tok // 2, HD), queries.dtype),
            pltpu.SemaphoreType.DMA((n - 1, 2)),
            pltpu.SemaphoreType.DMA((n - 1, 2)),
            pltpu.SemaphoreType.DMA((2, 2)),
        ],
        compiler_params=pltpu.CompilerParams(collective_id=1, has_side_effects=True),
        cost_estimate=pl.CostEstimate(flops=0, bytes_accessed=100_000_000, transcendentals=0),
        name="bring_back",
    )(of, os)
    terms = jnp.dot(attn, w_all, preferred_element_type=jnp.float32)
    return lax.psum_scatter(terms.astype(jnp.bfloat16), "head", scatter_dimension=1, tiled=True)


def body(n, queries, keys, values, frame_of_block, pair_mask, w_out):
    heads_here = queries.shape[1] // HD
    fits = n % 2 == 0 and 2 * heads_here == 3 * n and queries.shape[0] == 2 * BLK
    if fits:
        return body_spread(n, queries, keys, values, frame_of_block, pair_mask, w_out)
    return body_gather(queries, keys, values, frame_of_block, pair_mask, w_out)


def solution(mesh):
    placed = (
        P("seq", "head"),
        P("seq", "head"),
        P("seq", "head"),
        P("seq"),
        P("seq", None),
        P("head", "seq"),
    )
    return jax.shard_map(
        functools.partial(body, mesh.shape["seq"]), mesh=mesh, in_specs=placed, out_specs=P("seq", "head"), check_vma=False
    )
```

```python
import functools
import math

import jax
import jax.numpy as jnp
from jax import lax
from jax.experimental import pallas as pl
from jax.experimental.pallas import tpu as pltpu
from jax.sharding import PartitionSpec as P

HD = 128
BLK = 256
NEG = -1e30


def body_gather(queries, keys, values, frame_of_block, pair_mask, w_out):
    tok = queries.shape[0]
    heads_here = queries.shape[1] // HD
    count_blocks = pair_mask.shape[1]
    scale = 1.0 / math.sqrt(HD)
    key_span = 512
    q_heads = queries.reshape(tok, heads_here, HD)
    q_frame = jnp.repeat(frame_of_block, BLK)
    mask_rows = jnp.repeat(pair_mask.astype(jnp.float32), BLK, axis=0)
    block_ids = jnp.arange(count_blocks, dtype=jnp.int32)

    def update(state, k_rows, v_rows, allowed):
        peak, total, accum = state
        k_heads = k_rows.reshape(k_rows.shape[0], heads_here, HD)
        v_heads = v_rows.reshape(v_rows.shape[0], heads_here, HD)
        score = (
            jnp.einsum("qhd,khd->hqk", q_heads, k_heads, preferred_element_type=jnp.float32) * scale
        )
        score = jnp.where(allowed[None], score, -1e30)
        new_peak = jnp.maximum(peak, jnp.max(score, axis=2))
        weight = jnp.where(allowed[None], jnp.exp(score - new_peak[:, :, None]), 0.0)
        factor = jnp.exp(peak - new_peak)
        new_total = total * factor + jnp.sum(weight, axis=2)
        added = jnp.einsum(
            "hqk,khd->qhd", weight.astype(jnp.bfloat16), v_heads, preferred_element_type=jnp.float32
        )
        new_accum = accum * factor.T[:, :, None] + added
        return (new_peak, new_total, new_accum)

    def attend_block(state, k_rows, v_rows, k_frame, start):
        count = k_rows.shape[0]
        k_block = (start + jnp.arange(count, dtype=jnp.int32)) // BLK
        one_hot = (block_ids[:, None] == k_block[None, :]).astype(jnp.float32)
        link = jnp.dot(mask_rows, one_hot, preferred_element_type=jnp.float32)
        same = k_frame[None, :] == q_frame[:, None]
        allowed = (k_frame[None, :] <= q_frame[:, None]) & ((link > 0.5) | same)
        return update(state, k_rows, v_rows, allowed)

    initial = (
        jnp.full((heads_here, tok), -1e30, jnp.float32),
        jnp.zeros((heads_here, tok), jnp.float32),
        jnp.zeros((tok, heads_here, HD), jnp.float32),
    )
    k_frame_local = jnp.repeat(frame_of_block, BLK)
    k_rows = lax.all_gather(keys, "seq", axis=0, tiled=True)
    v_rows = lax.all_gather(values, "seq", axis=0, tiled=True)
    k_frame = lax.all_gather(k_frame_local, "seq", axis=0, tiled=True)
    count = k_rows.shape[0]

    def step(index, inner):
        offset = (index * key_span).astype(jnp.int32)
        return attend_block(
            inner,
            lax.dynamic_slice_in_dim(k_rows, offset, key_span, 0),
            lax.dynamic_slice_in_dim(v_rows, offset, key_span, 0),
            lax.dynamic_slice_in_dim(k_frame, offset, key_span, 0),
            offset,
        )

    state = lax.fori_loop(0, count // key_span, step, initial)
    peak, total, accum = state
    attn = (accum / total.T[:, :, None]).reshape(tok, heads_here * HD).astype(jnp.bfloat16)
    terms = jnp.dot(
        attn, lax.all_gather(w_out, "seq", axis=1, tiled=True), preferred_element_type=jnp.float32
    )
    return lax.psum_scatter(terms.astype(jnp.bfloat16), "head", scatter_dimension=1, tiled=True)


def greet(n, me):
    barrier = pltpu.get_barrier_semaphore()
    for k in range(1, n):
        pl.semaphore_signal(barrier, inc=1, device_id={"seq": lax.rem(me + k, n)}, device_id_type=pl.DeviceIdType.MESH)
    pl.semaphore_wait(barrier, n - 1)


def cols(head):
    return pl.ds(pl.multiple_of(head * HD, HD), HD)


def rows(start, size):
    return pl.ds(pl.multiple_of(start, size), size)


def spread_kernel(n, tok, q, k, v, meta, qf, qs, kf, ks, vf, vs, metas, hold, hold_half, hold_meta, send, recv, here):
    me = lax.axis_index("seq")
    half = tok // 2

    def pieces(to):
        pair, odd = to // 2, lax.rem(to, 2)
        own, shared = cols(3 * pair + 2 * odd), cols(3 * pair + 1)
        full = rows(me * tok, tok)
        return [
            (meta, metas.at[rows(me * 8, 8)]),
            (q.at[:, own], qf.at[full]),
            (k.at[:, own], kf.at[full]),
            (v.at[:, own], vf.at[full]),
            (q.at[rows(odd * half, half), shared], qs.at[rows(me * half, half)]),
            (k.at[:, shared], ks.at[full]),
            (v.at[:, shared], vs.at[full]),
        ]

    def bounce(index):
        if index == 0:
            return hold_meta
        if index == 4:
            return hold_half
        return hold.at[{1: 0, 2: 1, 3: 2, 5: 3, 6: 4}[index]]

    greet(n, me)
    copies = []
    for step in range(1, n):
        to = lax.rem(me + step, n)
        for i, (src, dst) in enumerate(pieces(to)):
            copy = pltpu.make_async_remote_copy(
                src_ref=src, dst_ref=dst, send_sem=send.at[step - 1, i], recv_sem=recv.at[step - 1, i],
                device_id={"seq": to}, device_id_type=pl.DeviceIdType.MESH,
            )
            copy.start()
            copies.append(copy)
    mine = pieces(me)
    ins = [pltpu.make_async_copy(src, bounce(i), here.at[0, i]) for i, (src, _) in enumerate(mine)]
    outs = [pltpu.make_async_copy(bounce(i), dst, here.at[1, i]) for i, (_, dst) in enumerate(mine)]
    for c in ins:
        c.start()
    for c, d in zip(ins, outs):
        c.wait()
        d.start()
    for d in outs:
        d.wait()
    for c in copies:
        c.wait()


def attend_kernel(first_pair, odd_ref, count_ref, list_ref, qf, qs, kf, ks, vf, vs, of, os):
    odd = odd_ref[0]
    j = pl.program_id(0) + first_pair
    factor = math.log2(math.e) / math.sqrt(HD)

    def scores(q, k):
        return lax.dot_general(q, k, (((1,), (1,)), ((), ())), preferred_element_type=jnp.float32)

    def fold(state, parts, vals):
        peak, total, accum = state
        top = parts[0]
        for s in parts[1:]:
            top = jnp.maximum(top, s)
        new_peak = jnp.maximum(peak, jnp.max(top, axis=1, keepdims=True))
        keep = jnp.exp2((peak - new_peak) * factor)
        total, accum = total * keep, accum * keep
        for s, v in zip(parts, vals):
            p = jnp.exp2((s - new_peak) * factor)
            for c in range(0, BLK, HD):
                total = total + p[:, c:c + HD]
            accum = accum + jnp.dot(p.astype(jnp.bfloat16), v, preferred_element_type=jnp.float32)
        return new_peak, total, accum

    def start():
        return (
            jnp.full((BLK, 1), NEG, jnp.float32),
            jnp.zeros((BLK, HD), jnp.float32),
            jnp.zeros((BLK, HD), jnp.float32),
        )

    def finish(state):
        _, total, accum = state
        return (accum / jnp.sum(total, axis=1, keepdims=True)).astype(jnp.bfloat16)

    def walk(block, streams):
        count = count_ref[block]

        def step(i, states):
            a = rows(list_ref[block, 2 * i] * BLK, BLK)
            b = rows(list_ref[block, 2 * i + 1] * BLK, BLK)
            bias = jnp.where(2 * i + 1 < count, 0.0, NEG).astype(jnp.float32)
            parts = [[scores(q, k[a, :]), scores(q, k[b, :]) + bias] for q, k, _ in streams]
            return tuple(
                fold(state, part, (v[a, :], v[b, :])) for state, part, (_, _, v) in zip(states, parts, streams)
            )

        return lax.fori_loop(0, (count + 1) // 2, step, tuple(start() for _ in streams))

    same, other = rows(odd * BLK, BLK), rows((1 - odd) * BLK, BLK)
    first, second = walk(2 * j + odd, [(qf[same, :], kf, vf), (qs[...], ks, vs)])
    of[same, :] = finish(first)
    os[...] = finish(second)
    (third,) = walk(2 * j + 1 - odd, [(qf[other, :], kf, vf)])
    of[other, :] = finish(third)


def project_kernel(pairs, whole_heads, shared_heads, w, out):
    parts = []
    for p in range(pairs):
        parts += [whole_heads[p, 0], shared_heads[p, 0], whole_heads[p, 1]]
    attn = jnp.concatenate(parts, axis=1)
    out[...] = jnp.dot(attn, w[...], preferred_element_type=jnp.float32).astype(out.dtype)


def body_spread(n, queries, keys, values, frame_of_block, pair_mask, w_out):
    tok, width = queries.shape
    count_blocks = pair_mask.shape[1]
    tokens = n * tok
    per = tok // BLK
    meta = jnp.concatenate([frame_of_block[:, None], pair_mask], axis=1)
    meta = jnp.pad(meta, ((0, 8 - per), (0, HD - 1 - count_blocks)))
    anyspace = pl.BlockSpec(memory_space=pl.ANY)
    big = jax.ShapeDtypeStruct((tokens, HD), queries.dtype)
    small = jax.ShapeDtypeStruct((tokens // 2, HD), queries.dtype)
    qf, qs, kf, ks, vf, vs, metas = pl.pallas_call(
        functools.partial(spread_kernel, n, tok),
        out_shape=[big, small, big, big, big, big, jax.ShapeDtypeStruct((8 * n, HD), jnp.int32)],
        in_specs=[anyspace] * 4,
        out_specs=[anyspace] * 7,
        scratch_shapes=[
            pltpu.VMEM((5, tok, HD), queries.dtype),
            pltpu.VMEM((tok // 2, HD), queries.dtype),
            pltpu.VMEM((8, HD), jnp.int32),
            pltpu.SemaphoreType.DMA((n - 1, 7)),
            pltpu.SemaphoreType.DMA((n - 1, 7)),
            pltpu.SemaphoreType.DMA((2, 7)),
        ],
        compiler_params=pltpu.CompilerParams(collective_id=0, has_side_effects=True),
        cost_estimate=pl.CostEstimate(flops=0, bytes_accessed=300_000_000, transcendentals=0),
        name="spread",
    )(queries, keys, values, meta)

    metas = metas.reshape(n, 8, HD)[:, :per].reshape(n * per, HD)
    frame, links = metas[:, 0], metas[:, 1:1 + count_blocks]
    allowed = (frame[None, :] <= frame[:, None]) & ((links == 1) | (frame[None, :] == frame[:, None]))
    place = jnp.cumsum(allowed.astype(jnp.int32), axis=1)
    count = place[:, -1]
    ids = jnp.arange(count_blocks, dtype=jnp.int32)
    hit = allowed[:, None, :] & (place[:, None, :] == ids[None, :, None] + 1)
    order = jnp.sum(jnp.where(hit, ids[None, None, :], 0), axis=2)
    odd = lax.rem(lax.axis_index("seq"), 2).reshape(1).astype(jnp.int32)

    smem = pl.BlockSpec(memory_space=pltpu.SMEM)
    whole = pl.BlockSpec((tokens, HD), lambda j: (0, 0))
    pairs = n // 2
    span = tokens // 2
    sums = []
    for part in range(2):
        first = part * pairs
        of, os = pl.pallas_call(
            functools.partial(attend_kernel, first),
            grid=(pairs,),
            out_shape=[
                jax.ShapeDtypeStruct((span, HD), queries.dtype),
                jax.ShapeDtypeStruct((span // 2, HD), queries.dtype),
            ],
            in_specs=[
                smem,
                smem,
                smem,
                pl.BlockSpec((2 * BLK, HD), lambda j, first=first: (j + first, 0)),
                pl.BlockSpec((BLK, HD), lambda j, first=first: (j + first, 0)),
                whole,
                whole,
                whole,
                whole,
            ],
            out_specs=[pl.BlockSpec((2 * BLK, HD), lambda j: (j, 0)), pl.BlockSpec((BLK, HD), lambda j: (j, 0))],
            compiler_params=pltpu.CompilerParams(vmem_limit_bytes=40 * 1024 * 1024),
            cost_estimate=pl.CostEstimate(
                flops=(1 + 2 * part) * 7_000_000_000, bytes_accessed=8_000_000, transcendentals=8_000_000
            ),
            name=f"attend_{part}",
        )(odd, count, order, qf, qs, kf, ks, vf, vs)
        count, of = lax.optimization_barrier((count, of))
        got = lax.all_gather(jnp.concatenate([of, os], axis=0), "seq", axis=0, tiled=True)
        got = got.reshape(pairs, 2, span + span // 2, HD)
        terms = pl.pallas_call(
            functools.partial(project_kernel, pairs),
            grid=(span // BLK,),
            out_shape=jax.ShapeDtypeStruct((span, w_out.shape[1]), queries.dtype),
            in_specs=[
                pl.BlockSpec((pairs, 2, BLK, HD), lambda b: (0, 0, b, 0)),
                pl.BlockSpec((pairs, 1, BLK, HD), lambda b: (0, lax.rem(b, 2), span // BLK + b // 2, 0)),
                pl.BlockSpec(w_out.shape, lambda b: (0, 0)),
            ],
            out_specs=pl.BlockSpec((BLK, w_out.shape[1]), lambda b: (b, 0)),
            compiler_params=pltpu.CompilerParams(vmem_limit_bytes=24 * 1024 * 1024),
            cost_estimate=pl.CostEstimate(
                flops=2 * span * width * w_out.shape[1], bytes_accessed=12_000_000, transcendentals=0
            ),
            name=f"project_{part}",
        )(got, got, w_out)
        sums.append(lax.psum_scatter(terms, "head", scatter_dimension=0, tiled=True))

    heads = n // 2
    at = lax.axis_index("seq")
    came = []
    for turn in range(2):
        perm = []
        for s in range(n):
            for h in range(heads):
                part = (s + turn) % 2
                perm.append((s * heads + h, (part * heads + h) * heads + s // 2))
        block = jnp.where(lax.rem(at + turn, 2) == 0, sums[0], sums[1])
        came.append(lax.ppermute(block, ("seq", "head"), perm))
    swap = at // heads == 1
    left = jnp.where(swap, came[1], came[0])
    right = jnp.where(swap, came[0], came[1])
    return jnp.concatenate([left, right], axis=1)


def body(n, heads_axis, queries, keys, values, frame_of_block, pair_mask, w_out):
    heads_here = queries.shape[1] // HD
    fits = n % 2 == 0 and 2 * heads_here == 3 * n and queries.shape[0] == 2 * BLK and 2 * heads_axis == n
    if fits:
        return body_spread(n, queries, keys, values, frame_of_block, pair_mask, w_out)
    return body_gather(queries, keys, values, frame_of_block, pair_mask, w_out)


def solution(mesh):
    placed = (
        P("seq", "head"),
        P("seq", "head"),
        P("seq", "head"),
        P("seq"),
        P("seq", None),
        P("head", "seq"),
    )
    return jax.shard_map(
        functools.partial(body, mesh.shape["seq"], mesh.shape["head"]), mesh=mesh, in_specs=placed, out_specs=P("seq", "head"), check_vma=False
    )
```
